32 devices in a mesh: px: 8 (over z, x), py: 4 (over y, core).
Axes of the slice: x: 2, y: 2, z: 4, core: 2. Of those that a mesh axis runs over, the one named last changes fastest.
Arguments:
- potential: float32 [256, 256, 256], P(('px', 'py')), may hold values from 0 to 1
- recovery: float32 [256, 256, 256], P(('px', 'py')), may hold values from 0 to 2
- stimulus: float32 [256, 256, 256], P(('px', 'py')), may hold values from -8 to 8
- conductivity: float32 [256, 256, 256], P('px', 'py'), may hold values from 0.2 to 5
Outputs:
- potential_next: float32 [256, 256, 256], P(('px', 'py'))
- recovery_next: float32 [256, 256, 256], P(('px', 'py'))
The draws below stay inside these ranges and needn't reach their ends.
All inputs are finite; a program needn't handle non-finite values.
Results may differ from the reference program's by a relative error of at most 0.0003.
Values sent between devices are 32-bit elements; how exact they have to be, the bound alone decides.
A program may use at most 128 MiB of HBM per device.

```python
import math
import jax
import jax.numpy as jnp

GX = 256
GY = 256
GZ = 256
ITERS = 4


def draw_stimulus(key, part):
    noise = jnp.clip(jax.random.normal(key, (GX, GY, GZ), jnp.float32), -4.0, 4.0) * 2.0
    return noise


def block_scale(rng, shape, split, low, high):
    level, own = 1.0, jax.random.fold_in(rng, 6)
    for axis_at, parts in split:
        heights = jnp.exp(jax.random.uniform(jax.random.fold_in(own, axis_at), (parts,), jnp.float32, low / len(split), high / len(split)))
        level = level * jnp.repeat(heights, shape[axis_at] // parts).reshape([-1 if axis == axis_at else 1 for axis in range(len(shape))])
    return level


def setup_inputs(seed: int = 0) -> dict:
    key_list = jax.random.split(jax.random.key(seed), 5)
    potential = jnp.clip(1.0 * jax.random.uniform(key_list[0], (GX, GY, GZ), jnp.float32) ** block_scale(key_list[0], (GX, GY, GZ), ((0, 32),), -0.2, 0.2), 0.0, 1.0)
    recovery = jnp.clip(2.0 * jax.random.uniform(key_list[1], (GX, GY, GZ), jnp.float32) ** block_scale(key_list[1], (GX, GY, GZ), ((0, 32),), -0.2, 0.2), 0.0, 2.0)
    stimulus = draw_stimulus(jax.random.fold_in(key_list[4], 71), 0)
    conductivity = jnp.clip(jnp.exp(math.log(5.0) - 3.218876 * jax.random.uniform(key_list[3], (GX, GY, GZ), jnp.float32) ** block_scale(key_list[3], (GX, GY, GZ), ((0, 8), (1, 4)), -0.2, 0.2)), 0.2, 5.0)
    return dict(potential=potential, recovery=recovery, stimulus=stimulus, conductivity=conductivity)


mass_rate = 0.01
mean_conduct = 1.0
excite_gain = 8.0
threshold = 0.15
base_rate = 0.002
rate_slope = 0.2
rate_shift = 0.3
time_step = 0.1


def face_conductance(conductivity):
    result_list = []
    for dimension in range(3):
        for offset in (-1, 1):
            result_list.append(0.5 * (conductivity + jnp.roll(conductivity, offset, dimension)))
    return result_list


def operate(field, conductance):
    result_sum = mass_rate * field
    position = 0
    for dimension in range(3):
        for offset in (-1, 1):
            result_sum = result_sum + conductance[position] * (field - jnp.roll(field, offset, dimension))
            position = position + 1
    return result_sum


def wave_term(length):
    modes = jnp.arange(length, dtype=jnp.int32).astype(jnp.float32)
    return 2.0 - 2.0 * jnp.cos((2.0 * math.pi / length) * modes)


def precondition(residual, symbol):
    spectrum = jnp.fft.fftn(residual)
    return jnp.real(jnp.fft.ifftn(spectrum / symbol)).astype(residual.dtype)


def reference(potential, recovery, stimulus, conductivity):
    drive = excite_gain * potential * (potential - threshold) * (1.0 - potential) - potential * recovery
    v_star = potential + time_step * (drive + stimulus)
    rate = base_rate + rate_slope * recovery / (potential + rate_shift)
    recovery_next = recovery + time_step * rate * (-recovery - excite_gain * potential * (potential - threshold - 1.0))
    conductance = face_conductance(conductivity)
    symbol = mass_rate + mean_conduct * (wave_term(GX)[:, None, None] + wave_term(GY)[None, :, None] + wave_term(GZ)[None, None, :])
    solution = v_star
    residual = mass_rate * v_star - operate(solution, conductance)
    precond = precondition(residual, symbol)
    direction = precond
    product_now = jnp.sum(residual * precond)
    for step in range(ITERS):
        image = operate(direction, conductance)
        alpha = product_now / jnp.sum(direction * image)
        solution = solution + alpha * direction
        residual = residual - alpha * image
        if step < ITERS - 1:
            precond = precondition(residual, symbol)
            product_next = jnp.sum(residual * precond)
            direction = precond + (product_next / product_now) * direction
            product_now = product_next
    return solution, recovery_next
```

```python
import math

import jax
import jax.numpy as jnp
import numpy as np
from jax import lax
from jax.sharding import PartitionSpec as P

ITERS = 4

mass_rate = 0.01
excite_gain = 8.0
threshold = 0.15
base_rate = 0.002
rate_slope = 0.2
rate_shift = 0.3
time_step = 0.1
AXES = ("px", "py")


def cas_table(length):
    steps = np.arange(length)
    angle = 2.0 * math.pi / length * (steps[:, None] * steps[None, :] % length)
    return np.cos(angle) + np.sin(angle)


def wave_term(length):
    return 2.0 - 2.0 * np.cos(2.0 * math.pi / length * np.arange(length))


def mode_tables(length_y, length_z):
    shift = mass_rate + wave_term(length_y)[:, None] + wave_term(length_z)[None, :]
    root = np.sqrt(shift * (4.0 + shift))
    rho = 2.0 / (2.0 + shift + root)
    scale = 1.0 / (root * length_y * length_z)
    return rho, scale


def local(potential, recovery, stimulus, conductivity):
    devices = lax.axis_size("px") * lax.axis_size("py")
    me = lax.axis_index(AXES)
    rows, length_y, length_z = potential.shape
    length_x = rows * devices
    forth = [(i, (i + 1) % devices) for i in range(devices)]
    back = [((i + 1) % devices, i) for i in range(devices)]
    drive = (
        excite_gain * potential * (potential - threshold) * (1.0 - potential) - potential * recovery
    )
    v_star = potential + time_step * (drive + stimulus)
    rate = base_rate + rate_slope * recovery / (potential + rate_shift)
    recovery_next = recovery + time_step * rate * (
        -recovery - excite_gain * potential * (potential - threshold - 1.0)
    )
    cond = lax.all_to_all(conductivity, "py", split_axis=0, concat_axis=1, tiled=True)

    def above(field):
        return lax.ppermute(field[:1], AXES, back)

    def below(field):
        return lax.ppermute(field[-1:], AXES, forth)

    cond_x = jnp.concatenate([below(cond), cond, above(cond)], 0)
    face_x = 0.5 * (cond_x[1:] + cond_x[:-1])
    face_y = 0.5 * (cond + jnp.roll(cond, -1, 1))
    face_z = 0.5 * (cond + jnp.roll(cond, -1, 2))

    def faces(field):
        padded = jnp.concatenate([below(field), field, above(field)], 0)
        flow_x = face_x * (padded[:-1] - padded[1:])
        flow_y = face_y * (field - jnp.roll(field, -1, 1))
        flow_z = face_z * (field - jnp.roll(field, -1, 2))
        return (
            (flow_x[1:] - flow_x[:-1])
            + (flow_y - jnp.roll(flow_y, 1, 1))
            + (flow_z - jnp.roll(flow_z, 1, 2))
        )

    rho64, scale64 = mode_tables(length_y, length_z)
    rho = jnp.asarray(rho64, jnp.float32)
    scale = jnp.asarray(scale64, jnp.float32)
    cas_y = jnp.asarray(cas_table(length_y), jnp.float32)
    cas_z = jnp.asarray(cas_table(length_z), jnp.float32)
    step_log = jnp.asarray(rows * np.log(rho64), jnp.float32)
    closing = jnp.asarray(1.0 / (1.0 - rho64**length_x), jnp.float32)
    part = length_y // devices
    step_log = lax.dynamic_slice_in_dim(step_log, me * part, part, 0)
    closing = lax.dynamic_slice_in_dim(closing, me * part, part, 0)
    order = np.arange(devices)
    gap = jnp.asarray((order[:, None] - 1 - order[None, :]) % devices, jnp.float32)

    def both(field):
        field = jnp.einsum("xyz,zk->xyk", field, cas_z, precision=lax.Precision.HIGH)
        return jnp.einsum("xyk,yq->xqk", field, cas_y, precision=lax.Precision.HIGH)

    def apply_inverse(residual):
        spectrum = both(residual)
        head = spectrum[rows - 1]
        tail = spectrum[0]
        for i in range(1, rows):
            head = head + rho**i * spectrum[rows - 1 - i]
            tail = tail + rho**i * spectrum[i]
        ends = jnp.stack([head, tail])[None]
        ends = lax.all_to_all(ends, AXES, split_axis=2, concat_axis=0, tiled=True)
        power = jnp.exp(gap[:, :, None, None] * step_log) * closing
        left = jnp.sum(power * ends[None, :, 0], 1)
        right = jnp.sum(jnp.swapaxes(power, 0, 1) * ends[None, :, 1], 1)
        carry = jnp.stack([left, right], 1)
        carry = lax.all_to_all(carry, AXES, split_axis=0, concat_axis=2, tiled=True)
        forward, backward = [None] * rows, [None] * rows
        value = carry[0, 0]
        for i in range(rows):
            value = spectrum[i] + rho * value
            forward[i] = value
        value = carry[0, 1]
        for i in reversed(range(rows)):
            backward[i] = rho * value
            value = spectrum[i] + backward[i]
        return both(jnp.stack([scale * (f + b) for f, b in zip(forward, backward)]))

    field = v_star
    residual = -faces(v_star)
    direction = image = gamma = alpha = None
    for step in range(ITERS):
        precond = apply_inverse(residual)
        applied = mass_rate * precond + faces(precond)
        sums = jnp.stack([jnp.sum(residual * precond), jnp.sum(applied * precond)])
        sums = jnp.sum(lax.all_gather(jnp.broadcast_to(sums[:, None], (2, 128)), AXES), 0)
        gamma_next, delta = sums[0, 0], sums[1, 0]
        if step == 0:
            alpha = gamma_next / delta
            direction, image = precond, applied
        else:
            beta = gamma_next / gamma
            alpha = gamma_next / (delta - beta * gamma_next / alpha)
            direction = precond + beta * direction
            image = applied + beta * image
        gamma = gamma_next
        field = field + alpha * direction
        residual = residual - alpha * image
    return (field, recovery_next)


def solution(mesh):
    in_specs = (
        P(AXES, None, None),
        P(AXES, None, None),
        P(AXES, None, None),
        P("px", "py", None),
    )
    out_specs = (P(AXES, None, None), P(AXES, None, None))
    return jax.shard_map(local, mesh=mesh, in_specs=in_specs, out_specs=out_specs, check_vma=False)
```

```python
import math

import jax
import jax.numpy as jnp
import numpy as np
from jax import lax
from jax.experimental import pallas as pl
from jax.experimental.pallas import tpu as pltpu
from jax.sharding import PartitionSpec as P

ITERS = 4

mass_rate = 0.01
excite_gain = 8.0
threshold = 0.15
base_rate = 0.002
rate_slope = 0.2
rate_shift = 0.3
time_step = 0.1
AXES = ("px", "py")


def cas_table(length):
    steps = np.arange(length)
    angle = 2.0 * math.pi / length * (steps[:, None] * steps[None, :] % length)
    return np.cos(angle) + np.sin(angle)


def wave_term(length):
    return 2.0 - 2.0 * np.cos(2.0 * math.pi / length * np.arange(length))


def mode_tables(length_y, length_z):
    shift = mass_rate + wave_term(length_y)[:, None] + wave_term(length_z)[None, :]
    root = np.sqrt(shift * (4.0 + shift))
    rho = 2.0 / (2.0 + shift + root)
    scale = 1.0 / (root * length_y * length_z)
    return rho, scale


def local(potential, recovery, stimulus, conductivity):
    devices = lax.axis_size("px") * lax.axis_size("py")
    me = lax.axis_index(AXES)
    rows, length_y, length_z = potential.shape
    length_x = rows * devices
    forth = [(i, (i + 1) % devices) for i in range(devices)]
    back = [((i + 1) % devices, i) for i in range(devices)]
    drive = (
        excite_gain * potential * (potential - threshold) * (1.0 - potential) - potential * recovery
    )
    v_star = potential + time_step * (drive + stimulus)
    rate = base_rate + rate_slope * recovery / (potential + rate_shift)
    recovery_next = recovery + time_step * rate * (
        -recovery - excite_gain * potential * (potential - threshold - 1.0)
    )
    cond = lax.all_to_all(conductivity, "py", split_axis=0, concat_axis=1, tiled=True)

    def above(field):
        return lax.ppermute(field[:1], AXES, back)

    def below(field):
        return lax.ppermute(field[-1:], AXES, forth)

    cond_x = jnp.concatenate([below(cond), cond, above(cond)], 0)
    face_x = 0.5 * (cond_x[1:] + cond_x[:-1])
    face_y = 0.5 * (cond + jnp.roll(cond, -1, 1))
    face_z = 0.5 * (cond + jnp.roll(cond, -1, 2))

    def faces(field):
        padded = jnp.concatenate([below(field), field, above(field)], 0)
        flow_x = face_x * (padded[:-1] - padded[1:])
        flow_y = face_y * (field - jnp.roll(field, -1, 1))
        flow_z = face_z * (field - jnp.roll(field, -1, 2))
        return (
            (flow_x[1:] - flow_x[:-1])
            + (flow_y - jnp.roll(flow_y, 1, 1))
            + (flow_z - jnp.roll(flow_z, 1, 2))
        )

    rho64, scale64 = mode_tables(length_y, length_z)
    rho = jnp.asarray(rho64, jnp.float32)
    scale = jnp.asarray(scale64, jnp.float32)
    cas_y = jnp.asarray(cas_table(length_y), jnp.float32)
    cas_z = jnp.asarray(cas_table(length_z), jnp.float32)
    step_log = jnp.asarray(rows * np.log(rho64), jnp.float32)
    closing = jnp.asarray(1.0 / (1.0 - rho64**length_x), jnp.float32)
    part = length_y // devices
    step_log = lax.dynamic_slice_in_dim(step_log, me * part, part, 0)
    closing = lax.dynamic_slice_in_dim(closing, me * part, part, 0)
    order = np.arange(devices)
    gap = jnp.asarray((order[:, None] - 1 - order[None, :]) % devices, jnp.float32)

    def both(field):
        field = jnp.einsum("xyz,zk->xyk", field, cas_z, precision=lax.Precision.HIGH)
        return jnp.einsum("xyk,yq->xqk", field, cas_y, precision=lax.Precision.HIGH)

    def apply_inverse(residual):
        spectrum = both(residual)
        head = spectrum[rows - 1]
        tail = spectrum[0]
        for i in range(1, rows):
            head = head + rho**i * spectrum[rows - 1 - i]
            tail = tail + rho**i * spectrum[i]
        ends = jnp.stack([head, tail])[None]
        ends = lax.all_to_all(ends, AXES, split_axis=2, concat_axis=0, tiled=True)
        power = jnp.exp(gap[:, :, None, None] * step_log) * closing
        left = jnp.sum(power * ends[None, :, 0], 1)
        right = jnp.sum(jnp.swapaxes(power, 0, 1) * ends[None, :, 1], 1)
        carry = jnp.stack([left, right], 1)
        carry = lax.all_to_all(carry, AXES, split_axis=0, concat_axis=2, tiled=True)
        forward, backward = [None] * rows, [None] * rows
        value = carry[0, 0]
        for i in range(rows):
            value = spectrum[i] + rho * value
            forward[i] = value
        value = carry[0, 1]
        for i in reversed(range(rows)):
            backward[i] = rho * value
            value = spectrum[i] + backward[i]
        return both(jnp.stack([scale * (f + b) for f, b in zip(forward, backward)]))

    field = v_star
    residual = -faces(v_star)
    direction = image = gamma = alpha = None
    for step in range(ITERS):
        precond = apply_inverse(residual)
        applied = mass_rate * precond + faces(precond)
        sums = jnp.stack([jnp.sum(residual * precond), jnp.sum(applied * precond)])
        sums = jnp.sum(lax.all_gather(jnp.broadcast_to(sums[:, None], (2, 128)), AXES), 0)
        gamma_next, delta = sums[0, 0], sums[1, 0]
        if step == 0:
            alpha = gamma_next / delta
            direction, image = precond, applied
        else:
            beta = gamma_next / gamma
            alpha = gamma_next / (delta - beta * gamma_next / alpha)
            direction = precond + beta * direction
            image = applied + beta * image
        gamma = gamma_next
        field = field + alpha * direction
        residual = residual - alpha * image
    return (field, recovery_next)


def split(table):
    high = table.astype(jnp.bfloat16)
    low = (table - high.astype(np.float64)).astype(jnp.bfloat16)
    return jnp.asarray(high), jnp.asarray(low)


def parts_of(block):
    high = block.astype(jnp.bfloat16)
    return high, (block - high.astype(jnp.float32)).astype(jnp.bfloat16)


def product(left, right):
    def dot(a, b):
        return jnp.dot(a, b, preferred_element_type=jnp.float32)

    return dot(left[0], right[1]) + dot(left[1], right[0]) + dot(left[0], right[0])


def kernel(
    v_ref, cond_in, yh_ref, yl_ref, zh_ref, zl_ref, rho_ref, scale_ref, sigma_ref, close_ref,
    u_ref,
    cond, face_x, face_y, face_z, res, dire, imag, z_ref, w_ref, spec, back_ref, power,
    ends, recv, sol, carry, mine, gath,
    c_send, c_recv, h_send, h_recv, e_send, e_recv, s_send, s_recv, g_send, g_recv,
):
    count_y = lax.axis_size("py")
    devices = lax.axis_size("px") * count_y
    my_y = lax.axis_index("py")
    me = lax.axis_index("px") * count_y + my_y
    rows, length_y, length_z = v_ref.shape
    part = length_y // devices
    wide_y = cond_in.shape[1]
    mesh_type = pl.DeviceIdType.MESH

    def device(index):
        return (index // count_y, index % count_y)

    def strip(index):
        return pl.ds(pl.multiple_of(index * part, part), part)

    def halo(buffer, base):
        left = (me + devices - 1) % devices
        right = (me + 1) % devices
        return (
            pltpu.make_async_remote_copy(
                buffer.at[1], buffer.at[rows + 1], h_send.at[base], h_recv.at[base],
                device_id=device(left), device_id_type=mesh_type,
            ),
            pltpu.make_async_remote_copy(
                buffer.at[rows], buffer.at[0], h_send.at[base + 1], h_recv.at[base + 1],
                device_id=device(right), device_id_type=mesh_type,
            ),
        )

    def start_all(make, count):
        def begin(k, _):
            make(k).start()
            return 0

        lax.fori_loop(1, count, begin, 0)

    def wait_all(make, count):
        def finish(k, _):
            make(k).wait()
            return 0

        lax.fori_loop(1, count, finish, 0)

    def cond_copy(k):
        other = (my_y + k) % count_y
        return pltpu.make_async_remote_copy(
            cond_in.at[pl.ds(other * rows, rows)],
            cond.at[pl.ds(1, rows), pl.ds(pl.multiple_of(my_y * wide_y, 8), wide_y), :],
            c_send.at[k], c_recv.at[k],
            device_id=(lax.axis_index("px"), other), device_id_type=mesh_type,
        )

    def ends_copy(k):
        other = (me + k) % devices
        return pltpu.make_async_remote_copy(
            ends.at[:, strip(other), :], recv.at[me], e_send.at[k], e_recv.at[k],
            device_id=device(other), device_id_type=mesh_type,
        )

    def carry_copy(k):
        other = (me + k) % devices
        return pltpu.make_async_remote_copy(
            sol.at[other], carry.at[:, strip(me), :], s_send.at[k], s_recv.at[k],
            device_id=device(other), device_id_type=mesh_type,
        )

    def gath_copy(k):
        other = (me + k) % devices
        return pltpu.make_async_remote_copy(
            mine, gath.at[me], g_send.at[k], g_recv.at[k],
            device_id=device(other), device_id_type=mesh_type,
        )

    def stencil(k, _):
        i = (k + 1) % rows
        here = z_ref[i + 1]
        total = face_x[i + 1] * (here - z_ref[i + 2]) - face_x[i] * (z_ref[i] - here)
        flow = face_y[i] * (here - pltpu.roll(here, length_y - 1, 0))
        total = total + (flow - pltpu.roll(flow, 1, 0))
        flow = face_z[i] * (here - pltpu.roll(here, length_z - 1, 1))
        w_ref[i] = total + (flow - pltpu.roll(flow, 1, 1))
        return 0

    start_all(cond_copy, count_y)
    for i in range(rows):
        z_ref[i + 1] = v_ref[i]
        u_ref[i] = v_ref[i]
    field_halo = halo(z_ref, 0)
    for copy in field_halo:
        copy.start()
    cond[pl.ds(1, rows), pl.ds(pl.multiple_of(my_y * wide_y, 8), wide_y), :] = cond_in[
        pl.ds(my_y * rows, rows)
    ]
    wait_all(cond_copy, count_y)
    cond_halo = halo(cond, 2)
    for copy in cond_halo:
        copy.start()

    def faces(i, _):
        here = cond[i + 1]
        face_y[i] = 0.5 * (here + pltpu.roll(here, length_y - 1, 0))
        face_z[i] = 0.5 * (here + pltpu.roll(here, length_z - 1, 1))
        return 0

    lax.fori_loop(0, rows, faces, 0)
    for copy in cond_halo + field_halo:
        copy.wait()

    def faces_along(i, _):
        face_x[i] = 0.5 * (cond[i] + cond[i + 1])
        return 0

    lax.fori_loop(0, rows + 1, faces_along, 0)
    lax.fori_loop(0, rows, stencil, 0)

    def first(i, _):
        res[i] = -w_ref[i]
        dire[i] = jnp.zeros((length_y, length_z), jnp.float32)
        imag[i] = jnp.zeros((length_y, length_z), jnp.float32)
        return 0

    lax.fori_loop(0, rows, first, 0)

    def iteration(step, scalars):
        gamma, alpha = scalars
        ends[...] = jnp.zeros_like(ends)
        power[...] = jnp.ones_like(power)

        def ahead(i, _):
            block = product(parts_of(res[i]), (zh_ref[...], zl_ref[...]))
            block = product((yh_ref[...], yl_ref[...]), parts_of(block))
            spec[i] = block
            rho = rho_ref[...]
            ends[0] = block + rho * ends[0]
            ends[1] = ends[1] + power[...] * block
            power[...] = power[...] * rho
            return 0

        lax.fori_loop(0, rows, ahead, 0)
        start_all(ends_copy, devices)
        recv[me] = ends[:, strip(me), :]
        wait_all(ends_copy, devices)

        sigma = sigma_ref[strip(me), :]
        close = close_ref[strip(me), :]
        zero = jnp.zeros_like(sigma)

        def sums(b, pair):
            return (
                recv[b, 0] + sigma * pair[0],
                recv[devices - 1 - b, 1] + sigma * pair[1],
            )

        pair = lax.fori_loop(0, devices, sums, (zero, zero), unroll=4)

        def place(b, pair):
            c = devices - 1 - b
            sol[b, 0] = pair[0]
            sol[c, 1] = pair[1]
            return sums(b, pair)

        lax.fori_loop(0, devices, place, (pair[0] * close, pair[1] * close), unroll=4)
        start_all(carry_copy, devices)
        carry[:, strip(me), :] = sol[me]
        wait_all(carry_copy, devices)

        def behind(j, _):
            i = rows - 1 - j
            value = rho_ref[...] * carry[1]
            back_ref[i] = value
            carry[1] = spec[i] + value
            return 0

        lax.fori_loop(0, rows, behind, 0)

        def inverse(i, _):
            value = spec[i] + rho_ref[...] * carry[0]
            carry[0] = value
            value = scale_ref[...] * (value + back_ref[i])
            value = product((yh_ref[...], yl_ref[...]), parts_of(value))
            z_ref[i + 1] = product(parts_of(value), (zh_ref[...], zl_ref[...]))
            return 0

        lax.fori_loop(0, rows, inverse, 0)
        copies = halo(z_ref, 0)
        for copy in copies:
            copy.start()
        lax.fori_loop(0, rows - 2, stencil, 0)
        for copy in copies:
            copy.wait()
        lax.fori_loop(rows - 2, rows, stencil, 0)

        mine[...] = jnp.zeros_like(mine)

        def fold(value):
            value = jnp.sum(value.reshape(length_y // 8, 8, length_z), 0)
            return sum(value[:, c : c + 128] for c in range(0, length_z, 128))

        def dots(i, _):
            z = z_ref[i + 1]
            applied = mass_rate * z + w_ref[i]
            w_ref[i] = applied
            mine[0] = mine[0] + fold(z * res[i])
            mine[1] = mine[1] + fold(z * applied)
            return 0

        lax.fori_loop(0, rows, dots, 0)
        start_all(gath_copy, devices)
        gath[me] = mine[...]
        wait_all(gath_copy, devices)
        total = jnp.sum(gath[...], 0)
        gamma_next = jnp.sum(total[0], keepdims=True)
        delta = jnp.sum(total[1], keepdims=True)
        beta = jnp.where(step == 0, 0.0, gamma_next / gamma)
        alpha_next = gamma_next / (delta - beta * gamma_next / alpha)

        def update(i, _):
            direction = z_ref[i + 1] + beta * dire[i]
            image = w_ref[i] + beta * imag[i]
            dire[i] = direction
            imag[i] = image
            u_ref[i] = u_ref[i] + alpha_next * direction
            res[i] = res[i] - alpha_next * image
            return 0

        lax.fori_loop(0, rows, update, 0)
        return gamma_next, alpha_next

    one = jnp.ones((1, 1), jnp.float32)
    lax.fori_loop(0, ITERS, iteration, (one, one))


def fused(potential, recovery, stimulus, conductivity):
    devices = lax.axis_size("px") * lax.axis_size("py")
    rows, length_y, length_z = potential.shape
    part = length_y // devices
    if part % 8 or length_z % 128 or conductivity.shape[1] % 8:
        return local(potential, recovery, stimulus, conductivity)
    drive = (
        excite_gain * potential * (potential - threshold) * (1.0 - potential) - potential * recovery
    )
    v_star = potential + time_step * (drive + stimulus)
    rate = base_rate + rate_slope * recovery / (potential + rate_shift)
    recovery_next = recovery + time_step * rate * (
        -recovery - excite_gain * potential * (potential - threshold - 1.0)
    )
    rho, scale = mode_tables(length_y, length_z)
    tables = split(cas_table(length_y)) + split(cas_table(length_z))
    tables += tuple(
        jnp.asarray(table, jnp.float32)
        for table in (rho, scale, rho**rows, 1.0 / (1.0 - rho ** (rows * devices)))
    )
    plane = (length_y, length_z)
    whole = (rows,) + plane

    def vmem(shape):
        return pltpu.VMEM(shape, jnp.float32)

    dma = pltpu.SemaphoreType.DMA
    padded = (rows + 2,) + plane
    slots = (devices, 2, part, length_z)
    field = pl.pallas_call(
        kernel,
        out_shape=jax.ShapeDtypeStruct(whole, jnp.float32),
        in_specs=[pl.BlockSpec(memory_space=pltpu.VMEM)] * 10,
        out_specs=pl.BlockSpec(memory_space=pltpu.VMEM),
        scratch_shapes=[
            vmem(padded), vmem((rows + 1,) + plane), vmem(whole), vmem(whole),
            vmem(whole), vmem(whole), vmem(whole), vmem(padded), vmem(whole),
            vmem(whole), vmem(whole), vmem(plane),
            vmem((2,) + plane), vmem(slots), vmem(slots), vmem((2,) + plane),
            vmem((2, 8, 128)), vmem((devices, 2, 8, 128)),
            dma((devices,)), dma((devices,)), dma((4,)), dma((4,)),
            dma((devices,)), dma((devices,)), dma((devices,)), dma((devices,)),
            dma((devices,)), dma((devices,)),
        ],
        compiler_params=pltpu.CompilerParams(
            has_side_effects=True, vmem_limit_bytes=56 * 1024 * 1024
        ),
    )(v_star, conductivity, *tables)
    return (field, recovery_next)


def solution(mesh):
    in_specs = (
        P(AXES, None, None),
        P(AXES, None, None),
        P(AXES, None, None),
        P("px", "py", None),
    )
    out_specs = (P(AXES, None, None), P(AXES, None, None))
    return jax.shard_map(fused, mesh=mesh, in_specs=in_specs, out_specs=out_specs, check_vma=False)
```
